256 devices in a mesh: section: 4 (over x_hi, core), expert: 64 (over x_lo, z, y).
Axes of the slice: x: 4 (x_hi: 2, x_lo: 2; x = x_hi * 2 + x_lo), y: 4, z: 8, core: 2. Of those that a mesh axis runs over, the one named last changes fastest.
Arguments:
- x_fwd: bfloat16 [4, 8192, 3584], P('section', 'expert'), may hold values from -6 to 6
- routes_fwd: int32 [4, 8192, 2], P('section', 'expert'), may hold values from 0 to 31, all different within a row; in each aligned block of 128 rows (0 to 127, 128 to 255, ..., all dimensions but the last counted through in order) at most 12 rows name the same one
- affinity_fwd: float32 [4, 8192, 2], P('section', 'expert'), may hold values from 0.1 to 1
- x_bwd: bfloat16 [4, 8192, 3584], P('section', 'expert'), may hold values from -6 to 6
- grad_bwd: bfloat16 [4, 8192, 3584], P('section', 'expert'), may hold values from -6 to 6
- routes_bwd: int32 [4, 8192, 2], P('section', 'expert'), may hold values from 0 to 31, all different within a row; in each aligned block of 128 rows (0 to 127, 128 to 255, ..., all dimensions but the last counted through in order) at most 12 rows name the same one
- affinity_bwd: float32 [4, 8192, 2], P('section', 'expert'), may hold values from 0.1 to 1
- up_weight: bfloat16 [4, 3584, 32768], P('section', None, 'expert'), may hold values from -0.09375 to 0.09375
- down_weight: bfloat16 [4, 32768, 3584], P('section', 'expert'), may hold values from -0.1875 to 0.1875
Outputs:
- fwd_next: bfloat16 [4, 8192, 3584], P('section', 'expert')
- bwd_next: bfloat16 [4, 8192, 3584], P('section', 'expert')
The draws below stay inside these ranges and needn't reach their ends.
Inputs may be any that keep to these rules, and one draw needn't show every extreme that they name: `routes_fwd`: each row names 2 different experts; in each section, among the 128 rows of one device (aligned blocks), no expert is named more than 12 times, a bound that some block reaches. `routes_bwd`: each row names 2 different experts; in each section, among the 128 rows of one device (aligned blocks), no expert is named more than 12 times, a bound that some block reaches.
All inputs are finite; a program needn't handle non-finite values.
Results may differ from the reference program's by a relative error of at most 0.0041.
Values may be sent and summed in bfloat16 or wider, within the bound.
A program may use at most 128 MiB of HBM per device.

```python
import math
import jax
import jax.numpy as jnp
import numpy as np
from jax import lax

D = 3584
HID = 1024
TOP = 2
TOK_DEV = 128
SECTIONS = 4
EXPERTS = 32
TOKENS = 8192
CAP = 12
N_EXPERT = 64


def steps_of(key, shape, split, least, high):
    level, own = 1.0, jax.random.fold_in(key, 6)
    for position, shards_of in split:
        steps = jnp.exp(jax.random.uniform(jax.random.fold_in(own, position), (shards_of,), jnp.float32, least / len(split), high / len(split)))
        level = level * jnp.repeat(steps, shape[position] // shards_of).reshape([-1 if axis == position else 1 for axis in range(len(shape))])
    return level


def assign_block(stream_key, own, number, rows, count, top, limit, lean):
    sequence = jax.random.permutation(stream_key, count)
    crowded, ordinary = portions_of(count, rows * top, limit, lean, True), portions_of(count, rows * top, limit, lean, False)
    places = jnp.arange(count)

    def named(tallies, rotation):
        used = int((tallies > 0).sum())
        fixed = max(1, used // 4)
        passed = fixed + (places - fixed + rotation * (used - fixed)) % max(1, count - fixed)
        return jnp.zeros((count,), jnp.int32).at[sequence[jnp.where(places < fixed, places, passed)]].set(jnp.asarray(tallies, jnp.int32))

    tallies = jnp.where(number % 4 == 0, named(crowded, number // 4), named(ordinary, number - number // 4 - 1))
    mixed = jax.random.permutation(jax.random.fold_in(own, 3), count)
    giver, sink = mixed[0:count // 2 * 2:2], mixed[1:count // 2 * 2:2]
    slack = jnp.minimum(tallies[giver] - 1, limit - tallies[sink]) // 2
    slack = jnp.where((giver == sequence[0]) | (sink == sequence[0]) | (tallies[sink] == 0), 0, jnp.maximum(slack, 0))
    passed = jax.random.randint(jax.random.fold_in(own, 4), (count // 2,), 0, 1 << 20) % (slack + 1)
    tallies = tallies.at[giver].add(-passed).at[sink].add(passed)
    labels = jnp.searchsorted(jnp.cumsum(tallies), jnp.arange(rows * top), side="right").astype(jnp.int32)
    listing = labels.reshape(top, rows).T
    listing = listing[jax.random.permutation(jax.random.fold_in(own, 1), rows)]
    rotation = jax.random.randint(jax.random.fold_in(own, 2), (rows, 1), 0, top)
    return jnp.take_along_axis(listing, (jnp.arange(top)[None, :] + rotation) % top, axis=1)


def portions_of(count, total, limit, skew, full):
    portions = [(1 << 20) // math.isqrt(standing ** skew) + 1 for standing in range(1, count + 1)]
    largest = limit if full else min(limit, max(-(-total // count), total * portions[0] // sum(portions)))
    least = 1 if total - largest >= count - 1 else 0
    holding, surplus = [largest] + [least] * (count - 1), total - largest - least * (count - 1)
    while surplus > 0:
        free = [i for i in range(1, count) if holding[i] < largest] or [i for i in range(1, count) if holding[i] < limit]
        whole, left = sum([portions[i] for i in free]), surplus
        for i in free:
            extra = min(limit - holding[i], max(1, left * portions[i] // whole), surplus)
            holding[i] = holding[i] + extra
            surplus = surplus - extra
    return np.array(holding)


def gaussian(key, dims, deviation, bound, split=(), kind=jnp.bfloat16):
    array = deviation * jax.random.normal(key, dims, jnp.float32)
    if split:
        array = array * steps_of(key, dims, split, -0.22, 0.18)
    return jnp.clip(array, -bound, bound).astype(kind)


def setup_inputs(seed: int = 0) -> dict:
    keys = jax.random.split(jax.random.key(seed), 10)
    x_fwd = gaussian(keys[0], (SECTIONS, TOKENS, D), 1.0, 6.0, ((0, 4), (1, 64)))
    routes_fwd_keys = jax.random.split(jax.random.fold_in(keys[1], 1), SECTIONS * TOKENS // TOK_DEV)
    routes_fwd_turns = jax.random.permutation(jax.random.fold_in(keys[1], 3), SECTIONS * TOKENS // TOK_DEV)
    routes_fwd = jax.vmap(lambda own, number: assign_block(jax.random.fold_in(keys[1], 2), own, number, TOK_DEV, EXPERTS, TOP, CAP, 2))(routes_fwd_keys, routes_fwd_turns).reshape((SECTIONS, TOKENS, TOP))
    affinity_fwd = jnp.clip(jnp.exp(math.log(1.0) - 2.3025851 * jax.random.uniform(keys[2], (SECTIONS, TOKENS, TOP), jnp.float32) ** steps_of(keys[2], (SECTIONS, TOKENS, TOP), ((0, 4), (1, 64)), -0.2, 0.2)), 0.1, 1.0)
    x_bwd = gaussian(keys[3], (SECTIONS, TOKENS, D), 1.0, 6.0, ((0, 4), (1, 64)))
    grad_bwd = gaussian(keys[4], (SECTIONS, TOKENS, D), 1.0, 6.0, ((0, 4), (1, 64)))
    routes_bwd_keys = jax.random.split(jax.random.fold_in(keys[5], 1), SECTIONS * TOKENS // TOK_DEV)
    routes_bwd_turns = jax.random.permutation(jax.random.fold_in(keys[5], 3), SECTIONS * TOKENS // TOK_DEV)
    routes_bwd = jax.vmap(lambda own, number: assign_block(jax.random.fold_in(keys[5], 2), own, number, TOK_DEV, EXPERTS, TOP, CAP, 2))(routes_bwd_keys, routes_bwd_turns).reshape((SECTIONS, TOKENS, TOP))
    affinity_bwd = jnp.clip(jnp.exp(math.log(1.0) - 2.3025851 * jax.random.uniform(keys[6], (SECTIONS, TOKENS, TOP), jnp.float32) ** steps_of(keys[6], (SECTIONS, TOKENS, TOP), ((0, 4), (1, 64)), -0.2, 0.2)), 0.1, 1.0)
    up_weight = gaussian(keys[7], (SECTIONS, D, EXPERTS * HID), D ** -0.5, 0.09375, ((0, 4), (2, 64)))
    down_weight = gaussian(keys[8], (SECTIONS, EXPERTS * HID, D), HID ** -0.5, 0.1875, ((0, 4), (1, 64)))
    return {"x_fwd": x_fwd, "routes_fwd": routes_fwd, "affinity_fwd": affinity_fwd, "x_bwd": x_bwd, "grad_bwd": grad_bwd, "routes_bwd": routes_bwd, "affinity_bwd": affinity_bwd, "up_weight": up_weight, "down_weight": down_weight}


def silu_grad(values):
    sigma = jax.nn.sigmoid(values)
    return sigma * (1.0 + values * (1.0 - sigma))

def expert_pass(rows_fwd, rows_saved, rows_grad, up_block, down_block):
    half_count = HID // 2
    sums_fwd = jnp.zeros((rows_fwd.shape[0], D), jnp.float32)
    sums_bwd = jnp.zeros((rows_fwd.shape[0], D), jnp.float32)
    for half_id in range(2):
        up_part = up_block[:, half_id * half_count:(half_id + 1) * half_count]
        down_part = down_block[half_id * half_count:(half_id + 1) * half_count, :]
        hidden = jax.nn.silu(jnp.dot(rows_fwd, up_part, preferred_element_type=jnp.float32)).astype(jnp.bfloat16)
        part_fwd = jnp.dot(hidden, down_part, preferred_element_type=jnp.float32).astype(jnp.bfloat16)
        pre_act = jnp.dot(rows_saved, up_part, preferred_element_type=jnp.float32)
        hidden_grad = jnp.dot(rows_grad, down_part.T, preferred_element_type=jnp.float32)
        pre_grad = (hidden_grad * silu_grad(pre_act)).astype(jnp.bfloat16)
        part_bwd = jnp.dot(pre_grad, up_part.T, preferred_element_type=jnp.float32).astype(jnp.bfloat16)
        sums_fwd = sums_fwd + part_fwd.astype(jnp.float32)
        sums_bwd = sums_bwd + part_bwd.astype(jnp.float32)
    return (sums_fwd.astype(jnp.bfloat16), sums_bwd.astype(jnp.bfloat16))

def combine(inputs, results, affinity):
    weights = affinity / lax.optimization_barrier(jnp.sum(affinity, -1, keepdims=True))
    routed = results.reshape(TOKENS, TOP, D).astype(jnp.float32)
    return (inputs.astype(jnp.float32) + lax.optimization_barrier(jnp.sum(weights[..., None] * routed, 1))).astype(jnp.bfloat16)

def reference(x_fwd, routes_fwd, affinity_fwd, x_bwd, grad_bwd, routes_bwd, affinity_bwd, up_weight, down_weight):
    total = TOKENS * TOP
    rows = N_EXPERT * CAP
    zero_row = jnp.zeros((1, D), jnp.bfloat16)
    layer_outs = []
    input_grads = []
    for section_id in range(SECTIONS):
        inputs_fwd = jnp.concatenate([x_fwd[section_id], zero_row], 0)
        inputs_saved = jnp.concatenate([x_bwd[section_id], zero_row], 0)
        inputs_grad = jnp.concatenate([grad_bwd[section_id], zero_row], 0)
        flat_fwd = routes_fwd[section_id].reshape(-1)
        flat_bwd = routes_bwd[section_id].reshape(-1)
        up_section = up_weight[section_id]
        down_section = down_weight[section_id]

        def one_expert(carry, expert_id):
            results_fwd, results_bwd = carry
            index_fwd = jnp.nonzero(flat_fwd == expert_id, size=rows, fill_value=total)[0].astype(jnp.int32)
            index_bwd = jnp.nonzero(flat_bwd == expert_id, size=rows, fill_value=total)[0].astype(jnp.int32)
            up_block = lax.dynamic_slice_in_dim(up_section, (expert_id * HID).astype(jnp.int32), HID, 1)
            down_block = lax.dynamic_slice_in_dim(down_section, (expert_id * HID).astype(jnp.int32), HID, 0)
            token_fwd = index_fwd // TOP
            token_bwd = index_bwd // TOP
            outs_fwd, outs_bwd = expert_pass(inputs_fwd[token_fwd], inputs_saved[token_bwd], inputs_grad[token_bwd], up_block, down_block)
            results_fwd = results_fwd.at[index_fwd].set(outs_fwd)
            results_bwd = results_bwd.at[index_bwd].set(outs_bwd)
            return ((results_fwd, results_bwd), None)
        start = jnp.zeros((total + 1, D), jnp.bfloat16)
        (results_fwd, results_bwd), _ = lax.scan(one_expert, (start, start), jnp.arange(EXPERTS, dtype=jnp.int32))
        layer_outs.append(combine(x_fwd[section_id], results_fwd[:total], affinity_fwd[section_id]))
        input_grads.append(combine(grad_bwd[section_id], results_bwd[:total], affinity_bwd[section_id]))
    layer_out = jnp.stack(layer_outs)
    input_grad = jnp.stack(input_grads)
    return (jnp.roll(layer_out, 1, 0), jnp.roll(input_grad, -1, 0))
```

```python
import jax
import jax.numpy as jnp
from jax import lax
from jax.sharding import PartitionSpec as P

AGAINST_ROWS = (((1,), (1,)), ((), ()))


def silu_grad(values):
    sigma = jax.nn.sigmoid(values)
    return sigma * (1.0 + values * (1.0 - sigma))


def slots_of(routes, experts, capacity):
    flat = routes.reshape(-1)
    onehot = (flat[:, None] == jnp.arange(experts, dtype=jnp.int32)[None, :]).astype(jnp.int32)
    before = jnp.cumsum(onehot, 0) - onehot
    position = jnp.sum(before * onehot, 1)
    return (flat * capacity + position).reshape(routes.shape)


def pick_matrix(slot_of, slots):
    grid = jnp.arange(slots, dtype=jnp.int32)[:, None, None]
    return jnp.any(grid == slot_of[None, :, :], -1).astype(jnp.bfloat16)


def combine(inputs, results, slot_of, affinity):
    slots = results.shape[0]
    weights = affinity / jnp.sum(affinity, -1, keepdims=True)
    grid = jnp.arange(slots, dtype=jnp.int32)[None, None, :]
    mix = jnp.sum(jnp.where(grid == slot_of[:, :, None], weights[:, :, None], 0.0), 1)
    high = mix.astype(jnp.bfloat16)
    low = (mix - high.astype(jnp.float32)).astype(jnp.bfloat16)
    total = jnp.dot(high, results, preferred_element_type=jnp.float32) + jnp.dot(
        low, results, preferred_element_type=jnp.float32
    )
    return (inputs.astype(jnp.float32) + total).astype(jnp.bfloat16)


def per_device(
    x_fwd, routes_fwd, affinity_fwd, x_bwd, grad_bwd, routes_bwd, affinity_bwd, up_weight, down_weight
):
    devices = lax.axis_size("expert")
    experts = devices // 2
    tokens = x_fwd.shape[1]
    width = x_fwd.shape[2]
    capacity = 3 * tokens * routes_fwd.shape[2] // devices
    slots = experts * capacity
    outer = [(e // 2) * 4 + (0 if e % 2 == 0 else 3) for e in range(experts)]
    inner = [(e // 2) * 4 + (1 if e % 2 == 0 else 2) for e in range(experts)]
    groups = [outer, inner]

    def exchange(block):
        pieces = block.reshape(experts, capacity // 4, 4, width)
        moved = lax.all_to_all(
            pieces, "expert", split_axis=0, concat_axis=0, axis_index_groups=groups, tiled=True
        )
        return moved.reshape(slots, width)

    swap = [(i, i ^ 1) for i in range(devices)]
    up_own, down_own = up_weight[0], down_weight[0]
    up_other = lax.ppermute(up_own, "expert", swap)
    down_other = lax.ppermute(down_own, "expert", swap)

    slot_fwd = slots_of(routes_fwd[0], experts, capacity)
    slot_bwd = slots_of(routes_bwd[0], experts, capacity)
    pick_fwd = pick_matrix(slot_fwd, slots)
    pick_bwd = pick_matrix(slot_bwd, slots)

    def taken(pick, rows):
        return jnp.dot(pick, rows, preferred_element_type=jnp.float32).astype(jnp.bfloat16)

    out_fwd = taken(pick_fwd, x_fwd[0])
    out_x = taken(pick_bwd, x_bwd[0])
    out_g = taken(pick_bwd, grad_bwd[0])
    rows_fwd = exchange(out_fwd)
    rows_x = exchange(out_x)
    rows_g = exchange(out_g)

    def dot(a, b):
        return jnp.dot(a, b, preferred_element_type=jnp.float32)

    def dot_t(a, b):
        return lax.dot_general(a, b, AGAINST_ROWS, preferred_element_type=jnp.float32)

    def forward_half(up, down):
        hidden = jax.nn.silu(dot(rows_fwd, up)).astype(jnp.bfloat16)
        return dot(hidden, down)

    def backward_half(up, down):
        pre = (dot_t(rows_g, down) * silu_grad(dot(rows_x, up))).astype(jnp.bfloat16)
        return dot_t(pre, up)

    done_fwd = (forward_half(up_own, down_own) + forward_half(up_other, down_other)).astype(jnp.bfloat16)
    back_fwd = exchange(done_fwd)
    done_bwd = (backward_half(up_own, down_own) + backward_half(up_other, down_other)).astype(jnp.bfloat16)
    back_bwd = exchange(done_bwd)

    layer_out = combine(x_fwd[0], back_fwd, slot_fwd, affinity_fwd[0])
    input_grad = combine(grad_bwd[0], back_bwd, slot_bwd, affinity_bwd[0])
    sections = lax.axis_size("section")
    fwd_next = lax.ppermute(layer_out[None], "section", [(i, (i + 1) % sections) for i in range(sections)])
    bwd_next = lax.ppermute(input_grad[None], "section", [(i, (i - 1) % sections) for i in range(sections)])
    return (fwd_next, bwd_next)


def solution(mesh):
    rows = P("section", "expert", None)
    return jax.shard_map(
        per_device,
        mesh=mesh,
        in_specs=(rows,) * 7 + (P("section", None, "expert"), rows),
        out_specs=(rows, rows),
        check_vma=False,
    )
```
